32 devices in a mesh: groups: 2 (over y), tensor: 4 (over z), seq: 2 (over x), section: 2 (over core).
Axes of the slice: x: 2, y: 2, z: 4, core: 2. Of those that a mesh axis runs over, the one named last changes fastest.
Arguments:
- attn_out: bfloat16 [768, 8192], P(('groups', 'seq'), ('tensor', 'section')), parts along dimension 0, may hold values from -6 to 6
- residual: bfloat16 [768, 8192], P(('groups', 'seq'), ('tensor', 'section')), parts along dimension 0, may hold values from -120 to 120
- out_weight: bfloat16 [8192, 8192], P(('tensor', 'section')), may hold values from -0.09375 to 0.09375
- norm_gain: bfloat16 [8192], replicated, may hold values from 0.099609375 to 1.8984375
- gate_up: bfloat16 [8192, 2, 16384], P(None, None, ('tensor', 'seq', 'section')), may hold values from -0.0625 to 0.0625
Outputs:
- stream: bfloat16 [768, 8192], P(('groups', 'seq'), ('tensor', 'section')), parts along dimension 0
- hidden: bfloat16 [768, 16384], P('groups', ('tensor', 'seq', 'section')), parts along dimension 0
The draws below stay inside these ranges and needn't reach their ends.
There are 2 independent parts, one for each index of `groups`. The reference program is written for one: setup_inputs(seed, part) draws one part's arguments, and reference() takes and returns one part's arrays. A program takes and returns all parts, laid end to end along the dimension named above; an argument that names none is the same for every part. Nothing has to cross between parts.
All inputs are finite; a program needn't handle non-finite values.
Results may differ from the reference program's by a relative error of at most 0.012.
Values may be sent and summed in bfloat16 or wider, within the bound.
No kernel may reach another device: no remote copies, remote signals or barrier semaphores. Data moves between devices by JAX's collectives and lax.ppermute only.
A program may use at most 192 MiB of HBM per device.

```python
import math
import jax
import jax.numpy as jnp
from jax import lax

D = 8192
FFW = 16384
ROWS = 384
N_TENSOR = 4
N_SECTION = 2


def draw_residual(key, part):
    first_key, second_key, third_key = jax.random.split(key, 3)
    column_ramp = jnp.exp(math.log(4.0) * jnp.arange(D, dtype=jnp.float32) / max(D - 1, 1))
    column_rough = jax.random.uniform(second_key, (D,), jnp.float32, 0.5, 1.5)
    row_scales = 0.3 * jnp.exp(jax.random.uniform(third_key, (ROWS, 1), jnp.float32, 0.0, math.log(10.0)))
    values_base = jnp.clip(jax.random.normal(first_key, (ROWS, D), jnp.float32), -6.0, 6.0)
    return (values_base * row_scales * column_ramp * column_rough).astype(jnp.bfloat16)


def with_spikes(array, rng, source, target, shards_of, factor):
    owner, partner = [(jnp.arange(array.shape[axis_at]) // (array.shape[axis_at] // shards_of)).reshape([-1 if axis == axis_at else 1 for axis in range(array.ndim)]) for axis_at in (source, target)]
    chosen = jax.random.permutation(rng, shards_of)[partner]
    strong = (owner == chosen) | (owner == (partner + shards_of // 2) % shards_of)
    return jnp.where(strong, factor * array, array)


def block_levels(own_key, dims, pieces, low, largest):
    gain, own = 1.0, jax.random.fold_in(own_key, 6)
    for dim, shards_of in pieces:
        draws = jnp.exp(jax.random.uniform(jax.random.fold_in(own, dim), (shards_of,), jnp.float32, low / len(pieces), largest / len(pieces)))
        gain = gain * jnp.repeat(draws, dims[dim] // shards_of).reshape([-1 if axis == dim else 1 for axis in range(len(dims))])
    return gain


def scatter_about(rng, dims, scale, reach, cuts=(), kind=jnp.bfloat16):
    drawn = jax.random.normal(rng, dims, jnp.float32) * scale
    if len(cuts) > 0:
        drawn = block_levels(rng, dims, cuts, -0.22, 0.18) * drawn
    return jnp.clip(drawn, min=-reach, max=reach).astype(kind)


def bell_draw_with(own_key, dims, width, reach, cuts, heavy, held_as=jnp.bfloat16):
    entries = width * jax.random.normal(own_key, dims, jnp.float32)
    if cuts:
        entries = entries * block_levels(own_key, dims, cuts, -0.22, 0.18)
    return jnp.clip(with_spikes(entries, jax.random.fold_in(own_key, 3), *heavy), -reach, reach).astype(held_as)


def setup_inputs(seed: int = 0, part: int = 0) -> dict:
    splits = jax.random.split(jax.random.key(seed), 6)
    part_splits = jax.random.split(jax.random.fold_in(splits[5], part), 6)
    attn_out = scatter_about(part_splits[0], (ROWS, D), 1.0, 6.0, ((0, 2), (1, 8)))
    residual = draw_residual(jax.random.fold_in(jax.random.fold_in(splits[5], part), 71), part)
    out_weight = bell_draw_with(splits[2], (D, D), D ** -0.5, 0.09375, ((0, 8),), (0, 1, 8, 2.0))
    norm_gain = jnp.clip(1.0 + 0.18 * jax.random.normal(splits[3], (D,), jnp.float32), 0.099609375, 1.8984375).astype(jnp.bfloat16)
    gate_up = scatter_about(splits[4], (D, 2, FFW), D ** -0.5, 0.0625, ((2, 16),))
    return dict(attn_out=attn_out, residual=residual, out_weight=out_weight, norm_gain=norm_gain, gate_up=gate_up)


epsilon = 1e-06

def tree_reduce(partials):
    current = partials
    while current.shape[0] > 1:
        current = (current[0::2].astype(jnp.float32) + current[1::2].astype(jnp.float32)).astype(jnp.bfloat16)
    return current[0]

def reference(attn_out, residual, out_weight, norm_gain, gate_up):
    shards = N_TENSOR * N_SECTION
    shard_width = D // shards
    col_block = math.gcd(D, 512)
    inputs_3d = attn_out.astype(jnp.float32).reshape(ROWS, shards, shard_width)
    columns = out_weight.reshape(D, D // col_block, col_block).transpose(1, 0, 2)

    def one_block(weight_cols):
        split_weight = weight_cols.astype(jnp.float32).reshape(shards, shard_width, col_block)
        partials = jnp.einsum('rpd,pdc->prc', inputs_3d, split_weight, precision=lax.Precision.HIGHEST).astype(jnp.bfloat16)
        return tree_reduce(partials)
    projected = lax.map(one_block, columns).transpose(1, 0, 2).reshape(ROWS, D)
    stream = (projected.astype(jnp.float32) + residual.astype(jnp.float32)).astype(jnp.bfloat16)
    stream_wide = stream.astype(jnp.float32)
    mean_square = lax.optimization_barrier(jnp.sum(stream_wide * stream_wide, axis=1, keepdims=True)) / D
    normed = (stream_wide * lax.rsqrt(mean_square + epsilon) * norm_gain.astype(jnp.float32)).astype(jnp.bfloat16)
    products = jnp.dot(normed, gate_up.reshape(D, 2 * FFW), preferred_element_type=jnp.float32).reshape(ROWS, 2, FFW)
    hidden = (jax.nn.silu(products[:, 0]) * products[:, 1]).astype(jnp.bfloat16)
    return (stream, hidden)
```

```python
import math

import jax
import jax.numpy as jnp
from jax import lax
from jax.experimental import pallas as pl
from jax.experimental.pallas import tpu as pltpu
from jax.sharding import PartitionSpec as P

EPSILON = 1e-06
BF16 = jnp.bfloat16
F32 = jnp.float32
LINE = ("tensor", "section")
RELAYOUT_CALLS = 4
LONGEST_LINE = 8


def tile_of(size, limit):
    return math.gcd(size, limit)


def project(scalars, attn_out, out_weight, width):
    rows, depth = attn_out.shape
    tile = tile_of(width, 512)
    tiles = width // tile

    def weight_at(j, t, s):
        first = jnp.where(s[2] > 0, s[0] * tiles + t, jnp.where(s[3] > 0, s[1] * tiles, 0))
        second = jnp.where(s[3] > 0, s[1] * tiles + t, jnp.where(s[2] > 0, (s[0] + 1) * tiles - 1, 0))
        return 0, jnp.where(j == 0, first, second)

    def body(s, x_ref, w_ref, keep_ref, send_ref):
        @pl.when((pl.program_id(0) == 0) & (s[2] > 0))
        def _():
            keep_ref[...] = jnp.dot(x_ref[...], w_ref[...], preferred_element_type=F32).astype(BF16)

        @pl.when((pl.program_id(0) == 1) & (s[3] > 0))
        def _():
            send_ref[...] = jnp.dot(x_ref[...], w_ref[...], preferred_element_type=F32).astype(BF16)

    return pl.pallas_call(
        body,
        grid_spec=pltpu.PrefetchScalarGridSpec(
            num_scalar_prefetch=1,
            grid=(2, tiles),
            in_specs=[
                pl.BlockSpec((rows, depth), lambda j, t, s: (0, 0)),
                pl.BlockSpec((depth, tile), weight_at),
            ],
            out_specs=[
                pl.BlockSpec((rows, tile), lambda j, t, s: (0, jnp.where(j == 0, t, tiles - 1))),
                pl.BlockSpec((rows, tile), lambda j, t, s: (0, jnp.where(j == 0, 0, t))),
            ],
        ),
        out_shape=[jax.ShapeDtypeStruct((rows, width), BF16)] * 2,
        compiler_params=pltpu.CompilerParams(vmem_limit_bytes=12 << 20),
        name="project",
    )(scalars, attn_out, out_weight)


def split_weight(gate_up, buffer, call, calls):
    depth, _, cols = gate_up.shape
    span = depth // calls
    tile = tile_of(span, 256)
    steps = span // tile

    def body(w_ref, *refs):
        refs[-1][...] = jnp.swapaxes(w_ref[...], 0, 1)

    operands = [gate_up]
    in_specs = [pl.BlockSpec((tile, 2, cols), lambda i: (call * steps + i, 0, 0))]
    aliases = {}
    if buffer is not None:
        operands.append(buffer)
        in_specs.append(pl.BlockSpec(memory_space=pl.ANY))
        aliases = {1: 0}
    return pl.pallas_call(
        body,
        grid=(steps,),
        in_specs=in_specs,
        out_specs=pl.BlockSpec((2, tile, cols), lambda i: (0, call * steps + i, 0)),
        out_shape=jax.ShapeDtypeStruct((2, depth, cols), BF16),
        input_output_aliases=aliases,
        compiler_params=pltpu.CompilerParams(vmem_limit_bytes=12 << 20),
        name="split_weight",
    )(*operands)


def gate_products(scalars, blocks, gain, weight, carry, final):
    chunks = len(blocks[0])
    rows, width = blocks[0][0].shape
    _, depth, cols = weight.shape
    tile = tile_of(width, 512)
    tiles = width // tile
    total = chunks * rows
    sides = len(blocks)

    def block_at(j, t, s):
        index = s[0] * tiles + t
        for side in range(sides - 1, -1, -1):
            others = [k for k in range(sides) if k != side]
            here = s[side] * tiles + t
            if others:
                other = others[0]
                stay = s[other] * tiles + (0 if side == 0 else tiles - 1)
                here = jnp.where(s[2 + side] > 0, here, jnp.where(s[2 + other] > 0, stay, 0))
            index = here if side == sides - 1 else jnp.where(j == side, here, index)
        return index

    def chunk_spec(side):
        def at(j, t, s):
            return 0, jnp.where(j == side, t, 0 if side else tiles - 1)

        return pl.BlockSpec((rows, tile), at)

    first = carry is None

    def body(s, *refs):
        refs = list(refs)
        x_refs = [[refs.pop(0) for _ in range(chunks)] for _ in range(sides)]
        gain_ref, w_ref = refs.pop(0), refs.pop(0)
        if not first:
            acc_in, sq_in = refs.pop(0), refs.pop(0)
        if final:
            out_ref, staged, acc, squares = refs
        else:
            acc, squares, staged = refs
        j, t = pl.program_id(0), pl.program_id(1)

        @pl.when((j == 0) & (t == 0))
        def _():
            if first:
                acc[...] = jnp.zeros_like(acc)
                squares[...] = jnp.zeros_like(squares)
            else:
                acc[...] = acc_in[...]
                squares[...] = sq_in[...]

        for side in range(sides):

            @pl.when((j == side) & (s[2 + side] > 0))
            def _():
                for chunk in range(chunks):
                    x = x_refs[side][chunk][...].astype(F32)
                    at = pl.ds(chunk * rows, rows)
                    squares[at, :] += jnp.sum(x * x, axis=1, keepdims=True)
                    staged[at, :] = (x * gain_ref[...]).astype(BF16)
                for half in range(2):
                    acc[half] += jnp.dot(staged[...], w_ref[half], preferred_element_type=F32)

        if final:

            @pl.when((j == sides - 1) & (t == tiles - 1))
            def _():
                for chunk in range(chunks):
                    at = pl.ds(chunk * rows, rows)
                    scale = lax.rsqrt(squares[at, :] / depth + EPSILON)
                    gate = acc[0, at, :] * scale
                    up = acc[1, at, :] * scale
                    out_ref[pl.ds(s[4 + chunk] * rows, rows), :] = (gate / (1.0 + jnp.exp(-gate)) * up).astype(BF16)

    acc_shape, sq_shape = (2, total, cols), (total, 1)
    operands = [*blocks[0]] + ([*blocks[1]] if sides > 1 else []) + [gain, weight]
    in_specs = [chunk_spec(side) for side in range(sides) for _ in range(chunks)] + [
        pl.BlockSpec((1, tile), lambda j, t, s: (0, block_at(j, t, s))),
        pl.BlockSpec((2, tile, cols), lambda j, t, s: (0, block_at(j, t, s), 0)),
    ]
    acc_spec = pl.BlockSpec(acc_shape, lambda j, t, s: (0, 0, 0))
    sq_spec = pl.BlockSpec(sq_shape, lambda j, t, s: (0, 0))
    aliases = {}
    if not first:
        if not final:
            aliases = {1 + len(operands): 0, 2 + len(operands): 1}
        operands += list(carry)
        in_specs += [acc_spec, sq_spec]
    scratch = [pltpu.VMEM((total, tile), BF16)]
    if final:
        out_shape = jax.ShapeDtypeStruct((total, cols), BF16)
        out_specs = pl.BlockSpec((total, cols), lambda j, t, s: (0, 0))
        scratch += [pltpu.VMEM(acc_shape, F32), pltpu.VMEM(sq_shape, F32)]
    else:
        out_shape = [jax.ShapeDtypeStruct(acc_shape, F32), jax.ShapeDtypeStruct(sq_shape, F32)]
        out_specs = [acc_spec, sq_spec]
    return pl.pallas_call(
        body,
        grid_spec=pltpu.PrefetchScalarGridSpec(
            num_scalar_prefetch=1, grid=(sides, tiles), in_specs=in_specs, out_specs=out_specs, scratch_shapes=scratch
        ),
        out_shape=out_shape,
        input_output_aliases=aliases,
        compiler_params=pltpu.CompilerParams(vmem_limit_bytes=32 << 20),
        name="gate_products",
    )(scalars, *operands)


def swap_cores(x):
    return lax.ppermute(x, "section", [(0, 1), (1, 0)])


def scalar_row(*values):
    return jnp.stack([jnp.asarray(v, jnp.int32) for v in values])


def long_line(attn_out, residual, out_weight, norm_gain, gate_up):
    size, position = lax.axis_size(LINE), lax.axis_index(LINE)
    row_count, shard = attn_out.shape
    blocked = jnp.dot(attn_out, out_weight, preferred_element_type=F32).astype(BF16).reshape(row_count, size, shard)
    for level in range(size.bit_length() - 1):
        paired = blocked.reshape(row_count, blocked.shape[1] // 2, 2, shard)
        bit = position >> level & 1
        kept = lax.dynamic_index_in_dim(paired, bit, 2, keepdims=False)
        sent = lax.dynamic_index_in_dim(paired, 1 - bit, 2, keepdims=False)
        received = lax.ppermute(sent, LINE, [(i, i ^ 1 << level) for i in range(size)])
        blocked = (kept.astype(F32) + received.astype(F32)).astype(BF16)
    stream = (blocked.reshape(row_count, shard).astype(F32) + residual.astype(F32)).astype(BF16)
    wide = lax.all_gather(stream, LINE, axis=1, tiled=True).astype(F32)
    depth, _, cols = gate_up.shape
    mean_square = jnp.sum(wide * wide, axis=1, keepdims=True) / depth
    normed = (wide * lax.rsqrt(mean_square + EPSILON) * norm_gain.astype(F32)).astype(BF16)
    normed = lax.all_gather(normed, "seq", axis=0, tiled=True)
    products = jnp.dot(normed, gate_up.reshape(depth, 2 * cols), preferred_element_type=F32)
    products = products.reshape(normed.shape[0], 2, cols)
    return stream, (jax.nn.silu(products[:, 0]) * products[:, 1]).astype(BF16)


def local(attn_out, residual, out_weight, norm_gain, gate_up):
    if lax.axis_size("tensor") > LONGEST_LINE:
        return long_line(attn_out, residual, out_weight, norm_gain, gate_up)
    line, cores, replicas = (lax.axis_size(name) for name in ("tensor", "section", "seq"))
    z, core, x = (lax.axis_index(name) for name in ("tensor", "section", "seq"))
    rows, shard = attn_out.shape
    width = shard * cores
    upward = core == 0

    def add(*terms):
        return sum(term.astype(F32) for term in terms).astype(BF16)

    received = None
    for r in range(1, line):
        up_block, down_block = (z - r) % line, (z + r) % line
        up_valid = (z <= r - 1).astype(jnp.int32)
        down_valid = (z >= line - r).astype(jnp.int32)
        keep_block, send_block = jnp.where(upward, up_block, down_block), jnp.where(upward, down_block, up_block)
        keep_valid, send_valid = jnp.where(upward, up_valid, down_valid), jnp.where(upward, down_valid, up_valid)
        keep, send = project(scalar_row(keep_block, send_block, keep_valid, send_valid), attn_out, out_weight, width)
        to_sibling = [(2 * k + 1, 2 * k) for k in range(r)] + [(2 * k, 2 * k + 1) for k in range(line - r, line)]
        other = lax.ppermute(send, LINE, to_sibling)
        terms = [keep, other] + ([received] if received is not None else [])
        pairs = [(2 * k, 2 * k + 2) for k in range(r)] + [(2 * k + 1, 2 * k - 1) for k in range(line - r, line)]
        received = lax.ppermute(add(*terms), LINE, pairs)
    own, _ = project(scalar_row(z, 0, 1, 0), attn_out, out_weight, width)
    total = add(own, received)
    mine = lax.dynamic_slice_in_dim(total, core * shard, shard, axis=1)
    theirs = swap_cores(lax.dynamic_slice_in_dim(total, (1 - core) * shard, shard, axis=1))
    stream = add(mine, theirs, residual)

    weight = None
    for call in range(RELAYOUT_CALLS):
        weight = split_weight(gate_up, weight, call, RELAYOUT_CALLS)
    gain = norm_gain.astype(F32).reshape(1, -1)

    def pair(a):
        b = swap_cores(a)
        return jnp.where(upward, jnp.concatenate([a, b], axis=1), jnp.concatenate([b, a], axis=1))

    def across(a, senders):
        out = []
        for shift in range(1, replicas):
            pairs = []
            for device in senders:
                for k in range(replicas):
                    there = (k + shift) % replicas
                    k_at, c_at = divmod(device, cores)
                    pairs.append(((k_at * replicas + k) * cores + c_at, (k_at * replicas + there) * cores + c_at))
            out.append(lax.ppermute(a, ("tensor", "seq", "section"), pairs))
        return out

    places = [(x - shift) % replicas for shift in range(replicas)]
    block = pair(stream)
    crossed = [pair(a) for a in across(stream, range(line * cores))]
    carry = gate_products(scalar_row(z, 0, 1, 0, *places), [[block, *crossed]], gain, weight, None, line == 1)
    moving = block
    for r in range(1, line):
        pairs = [(2 * k, 2 * k + 2) for k in range(r - 1, line - 1)]
        pairs += [(2 * k + 1, 2 * k - 1) for k in range(1, line - r + 1)]
        moving = lax.ppermute(moving, LINE, pairs)
        holders = [2 * k for k in range(r, line)] + [2 * k + 1 for k in range(0, line - r)]
        crossed = across(moving, holders)
        chunks = [moving, *crossed]
        others = [swap_cores(a) for a in chunks]
        below, above = z - r, z + r
        here, there = jnp.where(upward, below, above), jnp.where(upward, above, below)
        valid = [((b >= 0) & (b < line)).astype(jnp.int32) for b in (here, there)]
        scalars = scalar_row(here % line, there % line, *valid, *places)
        carry = gate_products(scalars, [chunks, others], gain, weight, carry, r == line - 1)
    return stream, carry


def solution(mesh):
    placed = (
        P(("groups", "seq"), ("tensor", "section")),
        P(("groups", "seq"), ("tensor", "section")),
        P(("tensor", "section"), None),
        P(),
        P(None, None, ("tensor", "seq", "section")),
    )
    return jax.shard_map(
        local,
        mesh=mesh,
        in_specs=placed,
        out_specs=(
            P(("groups", "seq"), ("tensor", "section")),
            P("groups", ("tensor", "seq", "section")),
        ),
        check_vma=False,
    )
```

```python
import math

import jax
import jax.numpy as jnp
import numpy as np
from jax import lax
from jax.experimental import pallas as pl
from jax.experimental.pallas import tpu as pltpu
from jax.sharding import PartitionSpec as P


EPSILON = 1e-06
BF16 = jnp.bfloat16
F32 = jnp.float32
LINE = ("tensor", "section")
RELAYOUT_CALLS = 4
LONGEST_LINE = 8
SMALL = 6 << 20
LARGE = 17 << 20


def tile_of(size, limit):
    return math.gcd(size, limit)


def hbm(x):
    return pltpu.with_memory_space_constraint(x, pltpu.HBM)


def vmem(x):
    return pltpu.with_memory_space_constraint(x, pltpu.VMEM)


def project(table, at, count, attn_out, out_weight, width):
    rows, depth = attn_out.shape
    tile = tile_of(width, 1024)
    tiles = width // tile

    def body(s, x_ref, w_ref, out_ref):
        out_ref[...] = jnp.dot(x_ref[...], w_ref[...], preferred_element_type=F32).astype(BF16)

    return pl.pallas_call(
        body,
        grid_spec=pltpu.PrefetchScalarGridSpec(
            num_scalar_prefetch=1,
            grid=(count, tiles),
            in_specs=[
                pl.BlockSpec((rows, depth), lambda j, t, s: (0, 0)),
                pl.BlockSpec((depth, tile), lambda j, t, s: (0, s[at + j] * tiles + t)),
            ],
            out_specs=pl.BlockSpec((None, rows, tile), lambda j, t, s: (j, 0, t)),
        ),
        out_shape=jax.ShapeDtypeStruct((count, rows, width), BF16),
        compiler_params=pltpu.CompilerParams(vmem_limit_bytes=12 << 20),
        name="project",
    )(table, attn_out, hbm(out_weight))


def add_up(terms):
    arrays = [term[0] if isinstance(term, tuple) else term for term in terms]
    rows, width = arrays[0].shape[-2:]
    tile = tile_of(width, 1024)
    specs = []
    for term in terms:
        if isinstance(term, tuple):
            specs.append(pl.BlockSpec((None, rows, tile), lambda t, k=term[1]: (k, 0, t)))
        else:
            specs.append(pl.BlockSpec((rows, tile), lambda t: (0, t)))

    def body(*refs):
        refs[-1][...] = sum(ref[...].astype(F32) for ref in refs[:-1]).astype(BF16)

    return pl.pallas_call(
        body,
        grid=(width // tile,),
        in_specs=specs,
        out_specs=pl.BlockSpec((rows, tile), lambda t: (0, t)),
        out_shape=jax.ShapeDtypeStruct((rows, width), BF16),
        compiler_params=pltpu.CompilerParams(vmem_limit_bytes=SMALL),
        name="add_up",
    )(*arrays)


def prepare(table, at, count, base, mine, theirs):
    rows, width = base.shape
    tile = tile_of(width, 1024)

    def plane(r, t, s):
        return jnp.maximum(s[at + r] - 1, 0), 0, t

    def body(s, base_ref, mine_ref, theirs_ref, out_ref):
        both = mine_ref[...].astype(F32) + theirs_ref[...].astype(F32)
        out_ref[...] = jnp.where(s[at + pl.program_id(0)] == 0, base_ref[...].astype(F32), both).astype(BF16)

    return pl.pallas_call(
        body,
        grid_spec=pltpu.PrefetchScalarGridSpec(
            num_scalar_prefetch=1,
            grid=(count, width // tile),
            in_specs=[pl.BlockSpec((rows, tile), lambda r, t, s: (0, t))] + [pl.BlockSpec((None, rows, tile), plane)] * 2,
            out_specs=pl.BlockSpec((None, rows, tile), lambda r, t, s: (r, 0, t)),
        ),
        out_shape=jax.ShapeDtypeStruct((count, rows, width), BF16),
        compiler_params=pltpu.CompilerParams(vmem_limit_bytes=SMALL),
        name="prepare",
    )(table, base, mine, theirs)


def pair(table, core_at, mine, theirs):
    rows, shard = mine.shape

    def body(s, mine_ref, theirs_ref, out_ref):
        core = s[core_at]

        @pl.when(core == 0)
        def _():
            out_ref[:, :shard] = mine_ref[...]
            out_ref[:, shard:] = theirs_ref[...]

        @pl.when(core != 0)
        def _():
            out_ref[:, :shard] = theirs_ref[...]
            out_ref[:, shard:] = mine_ref[...]

    spec = pl.BlockSpec((rows, shard), lambda i, s: (0, 0))
    return pl.pallas_call(
        body,
        grid_spec=pltpu.PrefetchScalarGridSpec(
            num_scalar_prefetch=1,
            grid=(1,),
            in_specs=[spec, spec],
            out_specs=pl.BlockSpec((rows, 2 * shard), lambda i, s: (0, 0)),
        ),
        out_shape=jax.ShapeDtypeStruct((rows, 2 * shard), BF16),
        compiler_params=pltpu.CompilerParams(vmem_limit_bytes=SMALL),
        name="pair",
    )(table, mine, theirs)


def finish_stream(table, core_at, mine, theirs, residual):
    rows, width = mine.shape
    shard = width // 2

    def body(s, mine_ref, theirs_ref, residual_ref, block_ref, half_ref):
        sums = mine_ref[...].astype(F32) + theirs_ref[...].astype(F32)
        block = (sums + residual_ref[...].astype(F32)).astype(BF16)
        block_ref[...] = block
        half_ref[...] = jnp.where(s[core_at] == 0, block[:, :shard], block[:, shard:])

    spec = pl.BlockSpec((rows, width), lambda i, s: (0, 0))
    return pl.pallas_call(
        body,
        grid_spec=pltpu.PrefetchScalarGridSpec(
            num_scalar_prefetch=1,
            grid=(1,),
            in_specs=[spec] * 3,
            out_specs=[spec, pl.BlockSpec((rows, shard), lambda i, s: (0, 0))],
        ),
        out_shape=[jax.ShapeDtypeStruct((rows, width), BF16), jax.ShapeDtypeStruct((rows, shard), BF16)],
        compiler_params=pltpu.CompilerParams(vmem_limit_bytes=SMALL),
        name="finish_stream",
    )(table, mine, theirs, residual)


def split_weight(gate_up, buffer, call, calls):
    depth, _, cols = gate_up.shape
    span = depth // calls
    tile = tile_of(span, 1024)
    steps = span // tile

    def body(w_ref, *refs):
        refs[-1][...] = jnp.swapaxes(w_ref[...], 0, 1)

    operands = [hbm(gate_up)]
    in_specs = [pl.BlockSpec((tile, 2, cols), lambda i: (call * steps + i, 0, 0))]
    aliases = {}
    if buffer is not None:
        operands.append(vmem(buffer))
        in_specs.append(pl.BlockSpec(memory_space=pl.ANY))
        aliases = {1: 0}
    return pl.pallas_call(
        body,
        grid=(steps,),
        in_specs=in_specs,
        out_specs=pl.BlockSpec((2, tile, cols), lambda i: (0, call * steps + i, 0)),
        out_shape=jax.ShapeDtypeStruct((2, depth, cols), BF16),
        input_output_aliases=aliases,
        compiler_params=pltpu.CompilerParams(vmem_limit_bytes=LARGE),
        name="split_weight",
    )(*operands)


def gate_products(table, at, places_at, blocks, gain, weight, carry, final):
    chunks = len(blocks[0])
    rows, width = blocks[0][0].shape
    _, depth, cols = weight.shape
    tile = tile_of(width, 1024)
    tiles = width // tile
    total = chunks * rows
    sides = len(blocks)

    def block_at(j, t, s):
        index = s[at] * tiles + t
        for side in range(sides - 1, -1, -1):
            others = [k for k in range(sides) if k != side]
            here = s[at + side] * tiles + t
            if others:
                other = others[0]
                stay = s[at + other] * tiles + (0 if side == 0 else tiles - 1)
                here = jnp.where(s[at + 2 + side] > 0, here, jnp.where(s[at + 2 + other] > 0, stay, 0))
            index = here if side == sides - 1 else jnp.where(j == side, here, index)
        return index

    def chunk_spec(side):
        def chunk_at(j, t, s):
            return 0, jnp.where(j == side, t, 0 if side else tiles - 1)

        return pl.BlockSpec((rows, tile), chunk_at)

    first = carry is None

    def body(s, *refs):
        refs = list(refs)
        x_refs = [[refs.pop(0) for _ in range(chunks)] for _ in range(sides)]
        gain_ref, w_ref = refs.pop(0), refs.pop(0)
        if not first:
            acc_in, sq_in = refs.pop(0), refs.pop(0)
        if final:
            out_ref, staged, acc, squares = refs
        else:
            acc, squares, _, staged = refs
        j, t = pl.program_id(0), pl.program_id(1)

        @pl.when((j == 0) & (t == 0))
        def _():
            if first:
                acc[...] = jnp.zeros_like(acc)
                squares[...] = jnp.zeros_like(squares)
            else:
                acc[...] = acc_in[...]
                squares[...] = sq_in[...]

        for side in range(sides):

            @pl.when((j == side) & (s[at + 2 + side] > 0))
            def _():
                for chunk in range(chunks):
                    x = x_refs[side][chunk][...].astype(F32)
                    span = pl.ds(chunk * rows, rows)
                    squares[span, :] += jnp.sum(x * x, axis=1, keepdims=True)
                    staged[span, :] = (x * gain_ref[...].astype(F32)).astype(BF16)
                at_row = pl.multiple_of((s[at + side] * tiles + t) * tile, tile)
                for half in range(2):
                    acc[half] += jnp.dot(staged[...], w_ref[half, pl.ds(at_row, tile), :], preferred_element_type=F32)

        if final:

            @pl.when((j == sides - 1) & (t == tiles - 1))
            def _():
                for chunk in range(chunks):
                    span = pl.ds(chunk * rows, rows)
                    scale = lax.rsqrt(squares[span, :] / depth + EPSILON)
                    gate = acc[0, span, :] * scale
                    up = acc[1, span, :] * scale
                    out_ref[pl.ds(s[places_at + chunk] * rows, rows), :] = (gate / (1.0 + jnp.exp(-gate)) * up).astype(BF16)

    acc_shape, sq_shape = (2, total, cols), (total, 1)
    operands = [*blocks[0]] + ([*blocks[1]] if sides > 1 else []) + [gain, vmem(weight)]
    in_specs = [chunk_spec(side) for side in range(sides) for _ in range(chunks)] + [
        pl.BlockSpec((1, tile), lambda j, t, s: (0, block_at(j, t, s))),
        pl.BlockSpec(memory_space=pltpu.VMEM),
    ]
    acc_spec = pl.BlockSpec(acc_shape, lambda j, t, s: (0, 0, 0))
    sq_spec = pl.BlockSpec(sq_shape, lambda j, t, s: (0, 0))
    aliases = {} if final else {len(operands): 2}
    if not first:
        if not final:
            aliases |= {1 + len(operands): 0, 2 + len(operands): 1}
        operands += list(carry)
        in_specs += [acc_spec, sq_spec]
    scratch = [pltpu.VMEM((total, tile), BF16)]
    if final:
        out_shape = jax.ShapeDtypeStruct((total, cols), BF16)
        out_specs = pl.BlockSpec((total, cols), lambda j, t, s: (0, 0))
        scratch += [pltpu.VMEM(acc_shape, F32), pltpu.VMEM(sq_shape, F32)]
    else:
        out_shape = [jax.ShapeDtypeStruct(shape, F32) for shape in (acc_shape, sq_shape)]
        out_shape.append(jax.ShapeDtypeStruct(weight.shape, BF16))
        out_specs = [acc_spec, sq_spec, pl.BlockSpec(memory_space=pl.ANY)]
    return pl.pallas_call(
        body,
        grid_spec=pltpu.PrefetchScalarGridSpec(
            num_scalar_prefetch=1, grid=(sides, tiles), in_specs=in_specs, out_specs=out_specs, scratch_shapes=scratch
        ),
        out_shape=out_shape,
        input_output_aliases=aliases,
        compiler_params=pltpu.CompilerParams(vmem_limit_bytes=LARGE - 4096),
        name="gate_products",
    )(table, *operands)


def swap_cores(x):
    return lax.ppermute(x, "section", [(0, 1), (1, 0)])


def layout_of(line, cores, replicas):
    order = [sorted((b for b in range(line) if b != k), key=lambda b: (-abs(b - k), -b)) + [k] for k in range(line)]
    rows = []
    for z in range(line):
        for core in range(cores):
            for x in range(replicas):
                row = list(order[z])
                for r in range(2, line):
                    up = order[z].index(z + line - r) if z < r else None
                    down = order[z].index(z - line + r) if z >= line - r else None
                    wanted = (up, down) if core == 0 else (down, up)
                    row.append(next((slot for slot in wanted if slot is not None), 0))
                row.append(core)
                row += [z, 0, 1, 0]
                for r in range(1, line):
                    pair_of = (z - r, z + r) if core == 0 else (z + r, z - r)
                    row += [b % line for b in pair_of] + [int(0 <= b < line) for b in pair_of]
                row += [(x - shift) % replicas for shift in range(replicas)]
                rows.append(row)
    starts = dict(order=0, slots=line, core=2 * line - 2, gates=2 * line - 1, places=6 * line - 1)
    return np.asarray(rows, np.int32), starts


def long_line(attn_out, residual, out_weight, norm_gain, gate_up):
    size, position = lax.axis_size(LINE), lax.axis_index(LINE)
    row_count, shard = attn_out.shape
    blocked = jnp.dot(attn_out, out_weight, preferred_element_type=F32).astype(BF16).reshape(row_count, size, shard)
    for level in range(size.bit_length() - 1):
        paired = blocked.reshape(row_count, blocked.shape[1] // 2, 2, shard)
        bit = position >> level & 1
        kept = lax.dynamic_index_in_dim(paired, bit, 2, keepdims=False)
        sent = lax.dynamic_index_in_dim(paired, 1 - bit, 2, keepdims=False)
        received = lax.ppermute(sent, LINE, [(i, i ^ 1 << level) for i in range(size)])
        blocked = (kept.astype(F32) + received.astype(F32)).astype(BF16)
    stream = (blocked.reshape(row_count, shard).astype(F32) + residual.astype(F32)).astype(BF16)
    wide = lax.all_gather(stream, LINE, axis=1, tiled=True).astype(F32)
    depth, _, cols = gate_up.shape
    mean_square = jnp.sum(wide * wide, axis=1, keepdims=True) / depth
    normed = (wide * lax.rsqrt(mean_square + EPSILON) * norm_gain.astype(F32)).astype(BF16)
    normed = lax.all_gather(normed, "seq", axis=0, tiled=True)
    products = jnp.dot(normed, gate_up.reshape(depth, 2 * cols), preferred_element_type=F32)
    products = products.reshape(normed.shape[0], 2, cols)
    return stream, (jax.nn.silu(products[:, 0]) * products[:, 1]).astype(BF16)


def local(attn_out, residual, out_weight, norm_gain, gate_up):
    if lax.axis_size("tensor") > LONGEST_LINE:
        return long_line(attn_out, residual, out_weight, norm_gain, gate_up)
    line, cores, replicas = (lax.axis_size(name) for name in ("tensor", "section", "seq"))
    z, core, x = (lax.axis_index(name) for name in ("tensor", "section", "seq"))
    _, shard = attn_out.shape
    width = shard * cores
    rows_of, starts = layout_of(line, cores, replicas)
    table = lax.dynamic_index_in_dim(jnp.asarray(rows_of), (z * cores + core) * replicas + x, 0, keepdims=False)
    core_at = starts["core"]

    first = project(table, 0, 1, attn_out, out_weight, width)
    first_pair = swap_cores(first)
    base = add_up([(first, 0), (first_pair, 0)])
    rest = project(table, 1, line - 1, attn_out, out_weight, width)
    rest_pair = swap_cores(rest)
    bases = prepare(table, starts["slots"], line - 2, base, rest, rest_pair)
    residual_pair = swap_cores(residual)
    residual = pair(table, core_at, residual, residual_pair)
    moving = base
    for r in range(1, line):
        pairs = [(2 * k, 2 * k + 2) for k in range(r)] + [(2 * k + 1, 2 * k - 1) for k in range(line - r, line)]
        received = lax.ppermute(moving, LINE, pairs)
        moving = add_up([(bases, r - 1) if r < line - 1 else (rest, line - 2), received])
    block, stream = finish_stream(table, core_at, moving, swap_cores(moving), residual)

    weight = None
    for call in range(RELAYOUT_CALLS):
        weight = split_weight(gate_up, weight, call, RELAYOUT_CALLS)
    gain = norm_gain.reshape(1, -1)

    def across(a, senders):
        out = []
        for shift in range(1, replicas):
            pairs = []
            for device in senders:
                for k in range(replicas):
                    there = (k + shift) % replicas
                    k_at, c_at = divmod(device, cores)
                    pairs.append(((k_at * replicas + k) * cores + c_at, (k_at * replicas + there) * cores + c_at))
            out.append(lax.ppermute(a, ("tensor", "seq", "section"), pairs))
        return out

    crossed = across(stream, range(line * cores))
    crossed = [pair(table, core_at, a, swap_cores(a)) for a in crossed]

    def gate(r, blocks, weight, carry):
        at = starts["gates"] + 4 * r
        return gate_products(table, at, starts["places"], blocks, gain, weight, carry, r == line - 1)

    *carry, weight = gate(0, [[block, *crossed]], weight, None)
    moving = block
    for r in range(1, line):
        pairs = [(2 * k, 2 * k + 2) for k in range(r - 1, line - 1)]
        pairs += [(2 * k + 1, 2 * k - 1) for k in range(1, line - r + 1)]
        moving = lax.ppermute(moving, LINE, pairs)
        holders = [2 * k for k in range(r, line)] + [2 * k + 1 for k in range(0, line - r)]
        crossed = across(moving, holders)
        other = swap_cores(moving)
        others = [swap_cores(a) for a in crossed]
        result = gate(r, [[moving, *crossed], [other, *others]], weight, carry)
        if r < line - 1:
            *carry, weight = result
    return stream, result


def solution(mesh):
    placed = (
        P(("groups", "seq"), ("tensor", "section")),
        P(("groups", "seq"), ("tensor", "section")),
        P(("tensor", "section"), None),
        P(),
        P(None, None, ("tensor", "seq", "section")),
    )
    return jax.shard_map(
        local,
        mesh=mesh,
        in_specs=placed,
        out_specs=(
            P(("groups", "seq"), ("tensor", "section")),
            P("groups", ("tensor", "seq", "section")),
        ),
        check_vma=False,
    )
```
